128 devices in a mesh: row: 4 (over x), col: 4 (over y_lo, core), layer: 8 (over y_hi, z).
Axes of the slice: x: 4, y: 4 (y_hi: 2, y_lo: 2; y = y_hi * 2 + y_lo), z: 4, core: 2. Of those that a mesh axis runs over, the one named last changes fastest.
Arguments:
- left_factor: float32 [6144, 8192], P('row', 'col'), may hold values from -6 to 6
- right_factor: float32 [8192, 6144], P('row', 'col'), may hold values from -0.0625 to 0.0625
Outputs:
- product: float32 [6144, 6144], P(('row', 'layer'), 'col')
The draws below stay inside these ranges and needn't reach their ends.
All inputs are finite; a program needn't handle non-finite values.
Results may differ from the reference program's by a relative error of at most 0.000073.
Values sent between devices are 32-bit elements; how exact they have to be, the bound alone decides.
A program may use at most 192 MiB of HBM per device.

```python
import jax
import jax.numpy as jnp
from jax import lax

K = 8192
M = 6144
NC = 6144


def spiked(drawn, stream_key, source, target, blocks, factor):
    def block_of(dim):
        return (jnp.arange(drawn.shape[dim]) // (drawn.shape[dim] // blocks)).reshape((-1,) + (1,) * (drawn.ndim - 1 - dim))

    one_side = jax.random.permutation(stream_key, blocks)[block_of(target)]
    second = (block_of(target) + blocks // 2) % blocks
    return jnp.where((block_of(source) == one_side) | (block_of(source) == second), factor * drawn, drawn)


def block_scale(rng, dims, split, least, top_value):
    gain = 1.0
    for position, shards_of in split:
        draws = jax.random.uniform(jax.random.fold_in(jax.random.fold_in(rng, 6), position), (shards_of,), jnp.float32, least / len(split), top_value / len(split))
        gain = gain * jnp.repeat(jnp.exp(draws), dims[position] // shards_of).reshape((-1,) + (1,) * (len(dims) - 1 - position))
    return gain


def gaussian(key, dims, scale, reach, pieces=(), held_as=jnp.bfloat16):
    drawn = scale * jax.random.normal(key, dims, jnp.float32)
    if pieces:
        drawn = drawn * block_scale(key, dims, pieces, -0.22, 0.18)
    return jnp.clip(drawn, -reach, reach).astype(held_as)


def noise_with(key, dims, spread, most, cuts, heavy, dtype=jnp.bfloat16):
    drawn = spread * jax.random.normal(key, dims, jnp.float32)
    if cuts:
        drawn = drawn * block_scale(key, dims, cuts, -0.22, 0.18)
    return jnp.clip(spiked(drawn, jax.random.fold_in(key, 3), *heavy), -most, most).astype(dtype)


def setup_inputs(seed: int = 0) -> dict:
    seeds = jax.random.split(jax.random.key(seed), 3)
    return {
        "left_factor": noise_with(seeds[0], (M, K), 1.0, 6.0, ((0, 4), (1, 4)), (1, 0, 4, 2.0), jnp.float32),
        "right_factor": gaussian(seeds[1], (K, NC), K ** -0.5, 0.0625, ((0, 4), (1, 4)), jnp.float32),
    }


def reference(left_factor, right_factor):
    return jnp.dot(left_factor, right_factor, precision=lax.Precision.HIGHEST, preferred_element_type=jnp.float32)
```

```python
import functools

import jax
import jax.numpy as jnp
from jax import lax
from jax.experimental import pallas as pl
from jax.experimental.pallas import tpu as pltpu
from jax.sharding import PartitionSpec as P

MESH = pl.DeviceIdType.MESH
RING = 4
WIDTHS = (256, 256, 256)


def split(x):
    high = x.astype(jnp.bfloat16)
    low = (x - high.astype(jnp.float32)).astype(jnp.bfloat16)
    return high, low


def kernel(
    a_hbm, b_hbm, out,
    a_buf, a_two, b_buf, b_high, b_low, part, hop_two, hop_one, final,
    a_local, a_core_s, a_core_r, a_y_s, a_y_r, a_relay_s, a_relay_r,
    b_local, b_s, b_r, b_relay_s, b_relay_r,
    two_s, two_r, one_s, one_r, swap_s, swap_r, keep,
):
    row, col, layer = lax.axis_index("row"), lax.axis_index("col"), lax.axis_index("layer")
    low_y, core = lax.div(col, 2), lax.rem(col, 2)
    high_y, z = lax.div(layer, RING), lax.rem(layer, RING)
    y = high_y * 2 + low_y

    def on_y(at):
        return (row, lax.rem(at, 2) * 2 + core, lax.div(at, 2) * RING + z)

    x_up = (lax.rem(row + 1, RING), col, layer)
    x_down = (lax.rem(row + RING - 1, RING), col, layer)
    y_up, y_down = on_y(lax.rem(y + 1, RING)), on_y(lax.rem(y + RING - 1, RING))
    z_up = (row, col, high_y * RING + lax.rem(z + 1, RING))
    z_down = (row, col, high_y * RING + lax.rem(z + RING - 1, RING))
    y_across = (row, col, (1 - high_y) * RING + z)
    twin = (row, low_y * 2 + 1 - core, layer)

    rows = part.shape[2]
    depth = b_buf.shape[0] // RING
    half_depth = depth // 2
    columns = b_buf.shape[1]
    chunks = []
    at = 0
    for width in WIDTHS:
        chunks.append((at, width))
        at += width
    assert at == columns

    def remote(src, dst, send, recv, device):
        return pltpu.make_async_remote_copy(
            src_ref=src, dst_ref=dst, send_sem=send, recv_sem=recv, device_id=device, device_id_type=MESH
        )

    def arrived(ref, send, recv):
        remote(ref, ref, send, recv, twin).wait_recv()

    sent = []

    def go(copy):
        copy.start()
        sent.append(copy)

    owners = [lax.rem(z + shift, RING) for shift in (2, 1, 3, 0)]
    k_at = pl.multiple_of(z * depth, depth)

    def a_source(step, half):
        first = pl.multiple_of(half * RING * rows + owners[step] * rows, rows)
        return a_hbm.at[pl.ds(first, rows), pl.ds(k_at, depth)]

    def a_place(step, half, quarter):
        return a_buf.at[step, half, :, pl.ds(pl.multiple_of(quarter * depth, depth), depth)]

    far_same = (1 - low_y) * 2 + core
    far_twin = (1 - low_y) * 2 + 1 - core
    near_twin = low_y * 2 + 1 - core

    def a_start(step):
        go(remote(a_source(step, 0), a_place(step, 0, col), a_y_s.at[step, 0], a_y_r.at[step, 0], y_up))
        go(remote(a_source(step, 1), a_place(step, 1, col), a_y_s.at[step, 1], a_y_r.at[step, 1], y_down))
        for half in range(2):
            pltpu.make_async_copy(a_source(step, half), a_place(step, half, col), a_local.at[step, half]).start()
            go(remote(a_source(step, half), a_place(step, half, col), a_core_s.at[step, half], a_core_r.at[step, half], twin))

    def a_relay(step):
        for half in range(2):
            here = a_place(step, half, far_same)
            arrived(here, a_y_s.at[step, half], a_y_r.at[step, half])
            go(remote(here, here, a_relay_s.at[step, half], a_relay_r.at[step, half], twin))

    def a_split(step):
        for half in range(2):
            pltpu.make_async_copy(a_source(step, half), a_place(step, half, col), a_local.at[step, half]).wait()
            arrived(a_place(step, half, near_twin), a_core_s.at[step, half], a_core_r.at[step, half])
            arrived(a_place(step, half, far_twin), a_relay_s.at[step, half], a_relay_r.at[step, half])

            @pl.loop(0, rows // 16)
            def _(tile):
                band = pl.ds(pl.multiple_of(tile * 16, 16), 16)
                high, low = split(a_buf[step, half, band, :])
                a_two[step, half, 0, band, :] = high
                a_two[step, half, 1, band, :] = low

    def b_source(chunk, part_of):
        first, width = chunks[chunk]
        return b_hbm.at[
            pl.ds(pl.multiple_of(z * depth + part_of * half_depth, half_depth), half_depth),
            pl.ds(pl.multiple_of(high_y * columns + first, 128), width),
        ]

    def b_place(chunk, part_of, quarter):
        first, width = chunks[chunk]
        return b_buf.at[
            pl.ds(pl.multiple_of(quarter * depth + part_of * half_depth, half_depth), half_depth), pl.ds(first, width)
        ]

    row_up, row_down = x_up[0], x_down[0]
    row_across = lax.rem(row + 2, RING)

    def b_keep(chunk):
        for part_of in range(2):
            pltpu.make_async_copy(
                b_source(chunk, part_of), b_place(chunk, part_of, row), b_local.at[chunk, part_of]
            ).start()

    def b_start(chunk):
        for turn in range(2):
            up, down = turn, 1 - turn
            go(remote(b_source(chunk, up), b_place(chunk, up, row), b_s.at[chunk, 0, up], b_r.at[chunk, 0, up], x_up))
            go(remote(b_source(chunk, down), b_place(chunk, down, row), b_s.at[chunk, 1, down], b_r.at[chunk, 1, down], x_down))

    def b_relay(chunk):
        here = b_place(chunk, 0, row_down)
        arrived(here, b_s.at[chunk, 0, 0], b_r.at[chunk, 0, 0])
        go(remote(here, here, b_relay_s.at[chunk, 0], b_relay_r.at[chunk, 0], x_up))
        here = b_place(chunk, 1, row_up)
        arrived(here, b_s.at[chunk, 1, 1], b_r.at[chunk, 1, 1])
        go(remote(here, here, b_relay_s.at[chunk, 1], b_relay_r.at[chunk, 1], x_down))

    def b_split(chunk):
        for part_of in range(2):
            pltpu.make_async_copy(
                b_source(chunk, part_of), b_place(chunk, part_of, row), b_local.at[chunk, part_of]
            ).wait()
            arrived(b_place(chunk, part_of, row_across), b_relay_s.at[chunk, part_of], b_relay_r.at[chunk, part_of])
        arrived(b_place(chunk, 1, row_down), b_s.at[chunk, 0, 1], b_r.at[chunk, 0, 1])
        arrived(b_place(chunk, 0, row_up), b_s.at[chunk, 1, 0], b_r.at[chunk, 1, 0])
        first, width = chunks[chunk]
        cols = pl.ds(first, width)

        @pl.loop(0, b_buf.shape[0] // 64)
        def _(tile):
            band = pl.ds(pl.multiple_of(tile * 64, 64), 64)
            high, low = split(b_buf[band, cols])
            b_high[band, cols] = high
            b_low[band, cols] = low

    def c_cols(chunk):
        first, width = chunks[chunk]
        return pl.ds(first, width)

    def multiply(chunk, step):
        cols = c_cols(chunk)

        @pl.loop(0, 2)
        def _(half):
            both = a_two[step, half].reshape(2 * rows, -1)
            by_high = jnp.dot(both, b_high[:, cols], preferred_element_type=jnp.float32)
            by_low = jnp.dot(a_two[step, half, 0], b_low[:, cols], preferred_element_type=jnp.float32)
            part[step, half, :, cols] = by_high[:rows] + (by_high[rows:] + by_low)

        if step == 0:
            go(remote(part.at[0, 0, :, cols], hop_two.at[0, :, cols], two_s.at[chunk, 0], two_r.at[chunk, 0], z_up))
            go(remote(part.at[0, 1, :, cols], hop_two.at[1, :, cols], two_s.at[chunk, 1], two_r.at[chunk, 1], z_down))
        if step == 1:
            c_send(chunk, 1, 1)
        if step == 2:
            c_send(chunk, 2, 0)

    def c_send(chunk, step, half):
        cols = c_cols(chunk)
        way, device = (0, z_up) if step == 1 else (1, z_down)
        go(remote(part.at[step, half, :, cols], hop_one.at[way, half, :, cols], one_s.at[chunk, way, half], one_r.at[chunk, way, half], device))

    def add(chunk, step):
        cols = c_cols(chunk)
        half = step - 1
        arrived(hop_two.at[half, :, cols], two_s.at[chunk, half], two_r.at[chunk, half])
        part[step, half, :, cols] += hop_two[half, :, cols]
        c_send(chunk, step, half)

    def out_cols(chunk, side):
        first, width = chunks[chunk]
        return out.at[:, pl.ds(pl.multiple_of(side * columns + first, 128), width)]

    def finish(chunk):
        cols = c_cols(chunk)
        for half in (1, 0):
            for way in range(2):
                arrived(hop_one.at[way, half, :, cols], one_s.at[chunk, way, half], one_r.at[chunk, way, half])
            final[half, :, cols] = part[3, half, :, cols] + hop_one[0, half, :, cols] + hop_one[1, half, :, cols]
        go(remote(final.at[1 - high_y, :, cols], out_cols(chunk, high_y), swap_s.at[chunk], swap_r.at[chunk], y_across))
        pltpu.make_async_copy(final.at[high_y, :, cols], out_cols(chunk, high_y), keep.at[chunk]).start()

    barrier = pltpu.get_barrier_semaphore()
    peers = (x_up, x_down, y_up, y_down, z_up, z_down, y_across, twin)
    for peer in peers:
        pl.semaphore_signal(barrier, inc=1, device_id=peer, device_id_type=MESH)
    pl.semaphore_wait(barrier, len(peers))

    b_start(0)
    for step in range(4):
        a_start(step)
    for chunk in range(len(chunks)):
        b_keep(chunk)

    b_relay(0)
    b_start(1)
    a_relay(0)
    a_split(0)
    a_relay(1)
    b_split(0)
    multiply(0, 0)
    a_split(1)
    multiply(0, 1)
    b_relay(1)
    b_start(2)
    add(0, 1)
    a_relay(2)
    a_split(2)
    multiply(0, 2)
    add(0, 2)
    a_relay(3)
    a_split(3)
    multiply(0, 3)
    b_split(1)
    multiply(1, 0)
    multiply(1, 1)
    multiply(1, 2)
    b_relay(2)
    add(1, 1)
    add(1, 2)
    finish(0)
    multiply(1, 3)
    finish(1)
    b_split(2)
    for step in range(4):
        multiply(2, step)
    add(2, 1)
    add(2, 2)
    finish(2)

    for copy in sent:
        copy.wait_send()
    for chunk in range(len(chunks)):
        arrived(out_cols(chunk, 1 - high_y), swap_s.at[chunk], swap_r.at[chunk])
        pltpu.make_async_copy(final.at[high_y, :, c_cols(chunk)], out_cols(chunk, high_y), keep.at[chunk]).wait()


def per_device(left_factor, right_factor):
    layers = lax.axis_size("layer")
    rows = left_factor.shape[0] // layers
    depth = left_factor.shape[1] // RING
    full_depth = left_factor.shape[1]
    columns = right_factor.shape[1] // 2
    count = len(WIDTHS)
    dma = pltpu.SemaphoreType.DMA
    f32, bf16 = jnp.float32, jnp.bfloat16
    return pl.pallas_call(
        kernel,
        out_shape=jax.ShapeDtypeStruct((rows, 2 * columns), f32),
        in_specs=[pl.BlockSpec(memory_space=pl.ANY)] * 2,
        out_specs=pl.BlockSpec(memory_space=pl.ANY),
        scratch_shapes=[
            pltpu.VMEM((4, 2, rows, full_depth), f32),
            pltpu.VMEM((4, 2, 2, rows, full_depth), bf16),
            pltpu.VMEM((full_depth, columns), f32),
            pltpu.VMEM((full_depth, columns), bf16),
            pltpu.VMEM((full_depth, columns), bf16),
            pltpu.VMEM((4, 2, rows, columns), f32),
            pltpu.VMEM((2, rows, columns), f32),
            pltpu.VMEM((2, 2, rows, columns), f32),
            pltpu.VMEM((2, rows, columns), f32),
            dma((4, 2)), dma((4, 2)), dma((4, 2)), dma((4, 2)), dma((4, 2)), dma((4, 2)), dma((4, 2)),
            dma((count, 2)), dma((count, 2, 2)), dma((count, 2, 2)), dma((count, 2)), dma((count, 2)),
            dma((count, 2)), dma((count, 2)), dma((count, 2, 2)), dma((count, 2, 2)),
            dma((count,)), dma((count,)), dma((count,)),
        ],
        compiler_params=pltpu.CompilerParams(
            collective_id=0, has_side_effects=True, vmem_limit_bytes=64000 * 1024
        ),
        name="product",
    )(left_factor, right_factor)


def solution(mesh):
    placed = (P("row", "col"), P("row", "col"))
    return jax.shard_map(
        per_device,
        mesh=mesh,
        in_specs=placed,
        out_specs=P(("row", "layer"), "col"),
        check_vma=False,
    )
```

```python
import functools

import jax
import jax.numpy as jnp
from jax import lax
from jax.experimental import pallas as pl
from jax.experimental.pallas import tpu as pltpu
from jax.sharding import PartitionSpec as P

MESH = pl.DeviceIdType.MESH
RING = 4
WIDTHS = (128,) * 6


def split(x):
    high = x.astype(jnp.bfloat16)
    low = (x - high.astype(jnp.float32)).astype(jnp.bfloat16)
    return high, low


def kernel(
    a_hbm, b_hbm, out,
    a_buf, a_two, b_buf, b_two, part, hop_two, hop_one, final,
    a_local, a_core_s, a_core_r, a_y_s, a_y_r, a_relay_s, a_relay_r,
    b_local, b_s, b_first, b_rest, b_relay_s,
    two_s, two_r, one_s, one_r, swap_s, swap_r, keep,
):
    row, col, layer = lax.axis_index("row"), lax.axis_index("col"), lax.axis_index("layer")
    low_y, core = lax.div(col, 2), lax.rem(col, 2)
    high_y, z = lax.div(layer, RING), lax.rem(layer, RING)
    y = high_y * 2 + low_y

    def on_y(at):
        return (row, lax.rem(at, 2) * 2 + core, lax.div(at, 2) * RING + z)

    x_up = (lax.rem(row + 1, RING), col, layer)
    x_down = (lax.rem(row + RING - 1, RING), col, layer)
    y_up, y_down = on_y(lax.rem(y + 1, RING)), on_y(lax.rem(y + RING - 1, RING))
    z_up = (row, col, high_y * RING + lax.rem(z + 1, RING))
    z_down = (row, col, high_y * RING + lax.rem(z + RING - 1, RING))
    y_across = (row, col, (1 - high_y) * RING + z)
    twin = (row, low_y * 2 + 1 - core, layer)

    rows = part.shape[2]
    depth = b_buf.shape[0] // RING
    half_depth = depth // 2
    columns = b_buf.shape[1]
    chunks = []
    at = 0
    for width in WIDTHS:
        chunks.append((at, width))
        at += width
    assert at == columns

    def remote(src, dst, send, recv, device):
        return pltpu.make_async_remote_copy(
            src_ref=src, dst_ref=dst, send_sem=send, recv_sem=recv, device_id=device, device_id_type=MESH
        )

    def arrived(ref, semaphore):
        remote(ref, ref, semaphore, semaphore, twin).wait_recv()

    def left(ref, semaphore):
        remote(ref, ref, semaphore, semaphore, twin).wait_send()

    def go(copy):
        copy.start()

    owners = [[lax.rem(z + shift, RING) for shift in shifts] for shifts in ((2, 2), (1, 3), (3, 1), (0, 0))]
    tall = rows // 2
    bands = (pl.ds(0, tall), pl.ds(tall, tall))
    k_at = pl.multiple_of(z * depth, depth)

    def a_source(step, half, band):
        first = half * RING * rows + owners[step][band] * rows + band * tall
        return a_hbm.at[pl.ds(pl.multiple_of(first, tall), tall), pl.ds(k_at, depth)]

    def a_place(step, half, band, quarter):
        return a_buf.at[step, half, band, pl.ds(pl.multiple_of(quarter * depth, depth), depth)]

    far_same = (1 - low_y) * 2 + core
    far_twin = (1 - low_y) * 2 + 1 - core
    near_twin = low_y * 2 + 1 - core

    def a_start(step):
        for band in range(2):
            for half, device in ((0, y_up), (1, y_down)):
                source, place = a_source(step, half, band), a_place(step, half, bands[band], col)
                go(remote(source, place, a_y_s, a_y_r.at[step, half], device))
                go(pltpu.make_async_copy(source, place, a_local.at[step]))
                go(remote(source, place, a_core_s, a_core_r.at[step], twin))

    def a_relay(step):
        for half in range(2):
            here = a_place(step, half, slice(None), far_same)
            arrived(here, a_y_r.at[step, half])
            go(remote(here, here, a_relay_s, a_relay_r.at[step], twin))

    def a_split(step):
        here = a_place(step, slice(None), slice(None), col)
        pltpu.make_async_copy(here, here, a_local.at[step]).wait()
        arrived(a_place(step, slice(None), slice(None), near_twin), a_core_r.at[step])
        arrived(a_place(step, slice(None), slice(None), far_twin), a_relay_r.at[step])
        for half in range(2):

            @pl.loop(0, rows // 16)
            def _(tile):
                band = pl.ds(pl.multiple_of(tile * 16, 16), 16)
                high, low = split(a_buf[step, half, band, :])
                a_two[step, half, 0, band, :] = high
                a_two[step, half, 1, band, :] = low

    def b_source(chunk, part_of):
        first, width = chunks[chunk]
        return b_hbm.at[
            pl.ds(pl.multiple_of(z * depth + part_of * half_depth, half_depth), half_depth),
            pl.ds(pl.multiple_of(high_y * columns + first, 128), width),
        ]

    def b_place(chunk, part_of, quarter):
        first, width = chunks[chunk]
        return b_buf.at[
            pl.ds(pl.multiple_of(quarter * depth + part_of * half_depth, half_depth), half_depth), pl.ds(first, width)
        ]

    row_up, row_down = x_up[0], x_down[0]
    row_across = lax.rem(row + 2, RING)

    def b_own(chunk):
        first, width = chunks[chunk]
        source = b_hbm.at[
            pl.ds(pl.multiple_of(z * depth, depth), depth), pl.ds(pl.multiple_of(high_y * columns + first, 128), width)
        ]
        place = b_buf.at[pl.ds(pl.multiple_of(row * depth, depth), depth), pl.ds(first, width)]
        return pltpu.make_async_copy(source, place, b_local.at[chunk])

    def b_keep(chunk):
        b_own(chunk).start()

    def b_start(chunk, turn):
        for way, part_of, device in ((0, turn, x_up), (1, 1 - turn, x_down)):
            arrival = b_first.at[chunk, way] if turn == 0 else b_rest.at[chunk, 0]
            go(remote(b_source(chunk, part_of), b_place(chunk, part_of, row), b_s, arrival, device))

    def b_relay(chunk):
        for way, quarter, device in ((0, row_down, x_up), (1, row_up, x_down)):
            here = b_place(chunk, way, quarter)
            arrived(here, b_first.at[chunk, way])
            go(remote(here, here, b_relay_s, b_rest.at[chunk, 1], device))

    def b_bands(chunk, shifts):
        first, width = chunks[chunk]
        for shift in shifts:
            start = lax.rem(row + shift, RING) * depth

            @pl.loop(0, depth // 64)
            def _(tile):
                band = pl.ds(pl.multiple_of(start + tile * 64, 64), 64)
                high, low = split(b_buf[band, pl.ds(first, width)])
                b_two[band, pl.ds(2 * first, width)] = high
                b_two[band, pl.ds(2 * first + width, width)] = low

    def b_split_near(chunk):
        first, width = chunks[chunk]
        b_own(chunk).wait()
        arrived(b_buf.at[pl.ds(0, depth), pl.ds(first, width)], b_rest.at[chunk, 0])
        b_bands(chunk, (0, 1, 3))

    def b_split_far(chunk):
        first, width = chunks[chunk]
        arrived(b_buf.at[pl.ds(0, depth), pl.ds(first, width)], b_rest.at[chunk, 1])
        b_bands(chunk, (2,))

    def b_split(chunk):
        b_split_near(chunk)
        b_split_far(chunk)

    def c_cols(chunk):
        first, width = chunks[chunk]
        return pl.ds(first, width)

    def groups(chunk):
        return ((0, 1 - high_y), (1, high_y)) if chunk >= len(chunks) - 2 else ((0, slice(None)),)

    def multiply(chunk, step):
        first, width = chunks[chunk]

        @pl.loop(0, 2)
        def _(half):
            both = a_two[step, half].reshape(2 * rows, -1)
            if width % 256:
                product = jnp.dot(both, b_two[:, pl.ds(2 * first, 2 * width)], preferred_element_type=jnp.float32)
                part[step, half, :, pl.ds(first, width)] = fold(product, width)
            else:
                by_high = jnp.dot(both, b_two[:, pl.ds(2 * first, width)], preferred_element_type=jnp.float32)
                by_low = jnp.dot(
                    a_two[step, half, 0], b_two[:, pl.ds(2 * first + width, width)], preferred_element_type=jnp.float32
                )
                part[step, half, :, pl.ds(first, width)] = by_high[:rows] + (by_high[rows:] + by_low)

        launch(chunk, step)

    def fold(product, width):
        small = product[:rows, width:] + (product[rows:, :width] + product[rows:, width:])
        return product[:rows, :width] + small

    def multiply_near(chunk, step, shifts=(0, 1, 3)):
        first, width = chunks[chunk]

        @pl.loop(0, 2)
        def _(half):
            product = 0.0
            for shift in shifts:
                inner = pl.ds(pl.multiple_of(lax.rem(row + shift, RING) * depth, depth), depth)
                both = a_two[step, half, :, :, inner].reshape(2 * rows, depth)
                product += jnp.dot(both, b_two[inner, pl.ds(2 * first, 2 * width)], preferred_element_type=jnp.float32)
            total = fold(product, width)
            if shifts == (2,):
                total += part[step, half, :, pl.ds(first, width)]
            part[step, half, :, pl.ds(first, width)] = total

    def multiply_far(chunk, step):
        multiply_near(chunk, step, (2,))
        launch(chunk, step)

    def launch(chunk, step):
        if step == 0:
            for group in groups(chunk)[: 1 if chunk == len(chunks) - 1 else 2]:
                far(chunk, group)
        if step == 2:
            near(chunk, 2, groups(chunk)[0])

    def far(chunk, group):
        turn, half = group
        cols = c_cols(chunk)
        for way, device in enumerate((z_up, z_down)):
            go(remote(
                part.at[0, half, bands[way], cols], hop_two.at[half, bands[way], cols],
                two_s, two_r.at[chunk, turn, way], device,
            ))

    def near(chunk, step, group, ways=(0, 1)):
        turn, half = group
        cols = c_cols(chunk)
        for way in ways:
            band, device = bands[way if step == 1 else 1 - way], (z_up, z_down)[way]
            go(remote(
                part.at[step, half, band, cols], hop_one.at[way, half, band, cols],
                one_s, one_r.at[chunk, turn], device,
            ))

    def add(chunk, turn=0):
        group = groups(chunk)[turn]
        half, cols = group[1], c_cols(chunk)
        for way in range(2):
            arrived(hop_two.at[half, bands[way], cols], two_r.at[chunk, turn, way])
            part[1, half, bands[way], cols] += hop_two[half, bands[way], cols]
            near(chunk, 1, group, (way,))

    def out_cols(chunk, side):
        first, width = chunks[chunk]
        return out.at[:, pl.ds(pl.multiple_of(side * columns + first, 128), width)]

    def finish(chunk, turn=0):
        cols = c_cols(chunk)
        half = groups(chunk)[turn][1]
        arrived(hop_one.at[:, half, :, cols], one_r.at[chunk, turn])
        final[half, :, cols] = part[3, half, :, cols] + hop_one[0, half, :, cols] + hop_one[1, half, :, cols]
        if turn == 0:
            go(remote(final.at[1 - high_y, :, cols], out_cols(chunk, high_y), swap_s, swap_r, y_across))
        if turn == len(groups(chunk)) - 1:
            pltpu.make_async_copy(final.at[high_y, :, cols], out_cols(chunk, high_y), keep).start()

    def settle():
        quarter = pl.ds(0, depth)
        left(a_buf.at[:, :, :, quarter], a_y_s)
        left(a_buf.at[:, :, :, quarter], a_core_s)
        left(a_buf.at[:, :, :, quarter], a_relay_s)
        left(b_buf.at[pl.ds(0, 2 * depth)], b_s)
        left(b_buf.at[quarter], b_relay_s)
        left(part.at[0], two_s)
        left(part.at[pl.ds(0, 2)], one_s)
        left(final.at[0], swap_s)
        mine = out.at[:, pl.ds(pl.multiple_of(high_y * columns, 128), columns)]
        theirs = out.at[:, pl.ds(pl.multiple_of((1 - high_y) * columns, 128), columns)]
        pltpu.make_async_copy(final.at[high_y], mine, keep).wait()
        arrived(theirs, swap_r)

    barrier = pltpu.get_barrier_semaphore()
    peers = (x_up, x_down, y_up, y_down, z_up, z_down, y_across, twin)
    for peer in peers:
        pl.semaphore_signal(barrier, inc=1, device_id=peer, device_id_type=MESH)
    pl.semaphore_wait(barrier, len(peers))

    b_start(0, 0)
    b_start(0, 1)
    b_start(1, 0)
    a_start(0)
    a_start(1)
    a_start(2)
    a_start(3)
    for chunk in range(len(chunks)):
        b_keep(chunk)

    b_relay(0)
    b_start(1, 1)
    b_start(2, 0)
    a_relay(0)
    b_relay(1)
    b_start(2, 1)
    b_start(3, 0)
    a_split(0)
    b_split(0)
    multiply(0, 0)
    a_relay(1)
    b_relay(2)
    b_start(3, 1)
    b_start(4, 0)
    b_split(1)
    multiply(1, 0)
    a_split(1)
    multiply(0, 1)
    add(0)
    multiply(1, 1)
    b_relay(3)
    b_start(4, 1)
    b_start(5, 0)
    a_relay(2)
    add(1)
    a_split(2)
    multiply(0, 2)
    multiply(1, 2)
    b_split(2)
    multiply(2, 0)
    multiply(2, 1)
    multiply(2, 2)
    a_relay(3)
    b_relay(4)
    b_start(5, 1)
    a_split(3)
    multiply(0, 3)
    add(2)
    b_split(3)
    multiply(3, 0)
    multiply(3, 1)
    multiply(3, 2)
    finish(0)
    multiply(1, 3)
    b_relay(5)
    multiply(2, 3)
    add(3)
    finish(1)
    b_split(4)
    multiply(4, 0)
    multiply(4, 1)
    multiply(4, 2)
    near(4, 2, groups(4)[1])
    multiply(3, 3)
    b_split_near(5)
    multiply_near(5, 0)
    finish(2)
    b_split_far(5)
    multiply_far(5, 0)
    add(4, 0)
    far(5, groups(5)[1])
    multiply(5, 1)
    multiply(5, 2)
    add(5, 0)
    add(4, 1)
    near(5, 2, groups(5)[1])
    multiply(4, 3)
    finish(3)
    finish(4, 0)
    add(5, 1)
    multiply(5, 3)
    finish(5, 0)
    finish(4, 1)
    finish(5, 1)

    settle()


def per_device(left_factor, right_factor):
    layers = lax.axis_size("layer")
    rows = left_factor.shape[0] // layers
    depth = left_factor.shape[1] // RING
    full_depth = left_factor.shape[1]
    columns = right_factor.shape[1] // 2
    count = len(WIDTHS)
    dma = pltpu.SemaphoreType.DMA
    f32, bf16 = jnp.float32, jnp.bfloat16
    return pl.pallas_call(
        kernel,
        out_shape=pltpu.VMEM((rows, 2 * columns), f32),
        in_specs=[pl.BlockSpec(memory_space=pl.ANY)] * 2,
        out_specs=pl.BlockSpec(memory_space=pl.ANY),
        scratch_shapes=[
            pltpu.VMEM((4, 2, rows, full_depth), f32),
            pltpu.VMEM((4, 2, 2, rows, full_depth), bf16),
            pltpu.VMEM((full_depth, columns), f32),
            pltpu.VMEM((full_depth, 2 * columns), bf16),
            pltpu.VMEM((4, 2, rows, columns), f32),
            pltpu.VMEM((2, rows, columns), f32),
            pltpu.VMEM((2, 2, rows, columns), f32),
            pltpu.VMEM((2, rows, columns), f32),
            dma((4,)), dma(()), dma((4,)), dma(()), dma((4, 2)), dma(()), dma((4,)),
            dma((count,)), dma(()), dma((count, 2)), dma((count, 2)), dma(()),
            dma(()), dma((count, 2, 2)), dma(()), dma((count, 2)), dma(()), dma(()), dma(()),
        ],
        compiler_params=pltpu.CompilerParams(
            collective_id=0, has_side_effects=True, vmem_limit_bytes=60000 * 1024
        ),
        name="product",
    )(left_factor, right_factor)


def solution(mesh):
    placed = (P("row", "col"), P("row", "col"))
    return jax.shard_map(
        per_device,
        mesh=mesh,
        in_specs=placed,
        out_specs=P(("row", "layer"), "col"),
        check_vma=False,
    )
```

```python
import functools

import jax
import jax.numpy as jnp
from jax import lax
from jax.experimental import pallas as pl
from jax.experimental.pallas import tpu as pltpu
from jax.sharding import PartitionSpec as P

MESH = pl.DeviceIdType.MESH
RING = 4
WIDTHS = (128,) * 6


def split(x):
    high = x.astype(jnp.bfloat16)
    low = (x - high.astype(jnp.float32)).astype(jnp.bfloat16)
    return high, low


def kernel(
    a_hbm, b_hbm, out,
    a_buf, a_two, b_buf, b_two, part, hop_two, hop_one, final,
    a_local, a_core_s, a_core_r, a_y_s, a_y_r, a_relay_s, a_relay_r,
    b_local, b_s, b_first, b_rest, b_relay_s,
    two_s, two_r, one_s, one_r, swap_s, swap_r, keep,
):
    row, col, layer = lax.axis_index("row"), lax.axis_index("col"), lax.axis_index("layer")
    low_y, core = lax.div(col, 2), lax.rem(col, 2)
    high_y, z = lax.div(layer, RING), lax.rem(layer, RING)
    y = high_y * 2 + low_y

    def on_y(at):
        return (row, lax.rem(at, 2) * 2 + core, lax.div(at, 2) * RING + z)

    x_up = (lax.rem(row + 1, RING), col, layer)
    x_down = (lax.rem(row + RING - 1, RING), col, layer)
    y_up, y_down = on_y(lax.rem(y + 1, RING)), on_y(lax.rem(y + RING - 1, RING))
    z_up = (row, col, high_y * RING + lax.rem(z + 1, RING))
    z_down = (row, col, high_y * RING + lax.rem(z + RING - 1, RING))
    y_across = (row, col, (1 - high_y) * RING + z)
    twin = (row, low_y * 2 + 1 - core, layer)

    rows = part.shape[2]
    depth = b_buf.shape[0] // RING
    half_depth = depth // 2
    columns = b_buf.shape[1]
    chunks = []
    at = 0
    for width in WIDTHS:
        chunks.append((at, width))
        at += width
    assert at == columns

    def remote(src, dst, send, recv, device):
        return pltpu.make_async_remote_copy(
            src_ref=src, dst_ref=dst, send_sem=send, recv_sem=recv, device_id=device, device_id_type=MESH
        )

    def arrived(ref, semaphore):
        remote(ref, ref, semaphore, semaphore, twin).wait_recv()

    def left(ref, semaphore):
        remote(ref, ref, semaphore, semaphore, twin).wait_send()

    def go(copy):
        copy.start()

    owners = [[lax.rem(z + shift, RING) for shift in shifts] for shifts in ((2, 2), (1, 3), (3, 1), (0, 0))]
    tall = rows // 2
    bands = (pl.ds(0, tall), pl.ds(tall, tall))
    k_at = pl.multiple_of(z * depth, depth)

    def a_source(step, half, band):
        first = half * RING * rows + owners[step][band] * rows + band * tall
        return a_hbm.at[pl.ds(pl.multiple_of(first, tall), tall), pl.ds(k_at, depth)]

    def a_place(step, half, band, quarter):
        return a_buf.at[step, half, band, pl.ds(pl.multiple_of(quarter * depth, depth), depth)]

    far_same = (1 - low_y) * 2 + core
    far_twin = (1 - low_y) * 2 + 1 - core
    near_twin = low_y * 2 + 1 - core

    def a_start(step):
        for band in range(2):
            for half, device in ((0, y_up), (1, y_down)):
                source, place = a_source(step, half, band), a_place(step, half, bands[band], col)
                go(remote(source, place, a_y_s, a_y_r.at[step, half, band], device))
                go(pltpu.make_async_copy(source, place, a_local))
                go(remote(source, place, a_core_s, a_core_r.at[step], twin))

    def a_relay(step, band):
        for half in range(2):
            here = a_place(step, half, bands[band], far_same)
            arrived(here, a_y_r.at[step, half, band])
            go(remote(here, here, a_relay_s, a_relay_r.at[step], twin))

    def a_split(step):
        if step == 0:
            here = a_buf.at[:, :, :, pl.ds(0, depth)]
            pltpu.make_async_copy(here, here, a_local).wait()
        arrived(a_place(step, slice(None), slice(None), near_twin), a_core_r.at[step])
        arrived(a_place(step, slice(None), slice(None), far_twin), a_relay_r.at[step])
        for half in range(2):

            @pl.loop(0, rows // 16)
            def _(tile):
                band = pl.ds(pl.multiple_of(tile * 16, 16), 16)
                high, low = split(a_buf[step, half, band, :])
                a_two[step, half, 0, band, :] = high
                a_two[step, half, 1, band, :] = low

    def b_source(chunk, part_of):
        first, width = chunks[chunk]
        return b_hbm.at[
            pl.ds(pl.multiple_of(z * depth + part_of * half_depth, half_depth), half_depth),
            pl.ds(pl.multiple_of(high_y * columns + first, 128), width),
        ]

    def b_place(chunk, part_of, quarter):
        first, width = chunks[chunk]
        return b_buf.at[
            pl.ds(pl.multiple_of(quarter * depth + part_of * half_depth, half_depth), half_depth), pl.ds(first, width)
        ]

    row_up, row_down = x_up[0], x_down[0]
    row_across = lax.rem(row + 2, RING)

    def b_own():
        source = b_hbm.at[
            pl.ds(pl.multiple_of(z * depth, depth), depth), pl.ds(pl.multiple_of(high_y * columns, 128), columns)
        ]
        place = b_buf.at[pl.ds(pl.multiple_of(row * depth, depth), depth), :]
        return pltpu.make_async_copy(source, place, b_local)

    def b_keep():
        b_own().start()

    def b_start(chunk, turn):
        for way, part_of, device in ((0, turn, x_up), (1, 1 - turn, x_down)):
            arrival = b_first.at[chunk, way] if turn == 0 else b_rest.at[chunk]
            go(remote(b_source(chunk, part_of), b_place(chunk, part_of, row), b_s, arrival, device))

    def b_relay(chunk):
        for way, quarter, device in ((0, row_down, x_up), (1, row_up, x_down)):
            here = b_place(chunk, way, quarter)
            arrived(here, b_first.at[chunk, way])
            go(remote(here, here, b_relay_s, b_rest.at[chunk + chunk // (len(chunks) - 1)], device))

    def b_bands(chunk, shifts):
        first, width = chunks[chunk]
        for shift in shifts:
            start = lax.rem(row + shift, RING) * depth

            @pl.loop(0, depth // 64)
            def _(tile):
                band = pl.ds(pl.multiple_of(start + tile * 64, 64), 64)
                high, low = split(b_buf[band, pl.ds(first, width)])
                b_two[band, pl.ds(2 * first, width)] = high
                b_two[band, pl.ds(2 * first + width, width)] = low

    def b_split_near(chunk):
        first, width = chunks[chunk]
        arrived(b_buf.at[pl.ds(0, depth), pl.ds(first, width)], b_rest.at[chunk])
        b_bands(chunk, (0, 1, 3))

    def b_split_far(chunk):
        first, width = chunks[chunk]
        arrived(b_buf.at[pl.ds(0, depth), pl.ds(first, width)], b_rest.at[chunk + 1])
        b_bands(chunk, (2,))

    def b_split(chunk):
        first, width = chunks[chunk]
        if chunk == 0:
            b_own().wait()
        arrived(b_buf.at[pl.ds(0, 2 * depth), pl.ds(first, width)], b_rest.at[chunk])
        b_bands(chunk, range(RING))

    def place_of(chunk, turn):
        return chunk + turn + max(0, chunk - (len(chunks) - 2))

    def c_cols(chunk):
        first, width = chunks[chunk]
        return pl.ds(first, width)

    def groups(chunk):
        return ((0, 1 - high_y), (1, high_y)) if chunk >= len(chunks) - 2 else ((0, slice(None)),)

    def multiply(chunk, step):
        first, width = chunks[chunk]

        for half in range(2):
            both = a_two[step, half].reshape(2 * rows, -1)
            if width % 256:
                product = jnp.dot(both, b_two[:, pl.ds(2 * first, 2 * width)], preferred_element_type=jnp.float32)
                part[step, half, :, pl.ds(first, width)] = fold(product, width)
            else:
                by_high = jnp.dot(both, b_two[:, pl.ds(2 * first, width)], preferred_element_type=jnp.float32)
                by_low = jnp.dot(
                    a_two[step, half, 0], b_two[:, pl.ds(2 * first + width, width)], preferred_element_type=jnp.float32
                )
                part[step, half, :, pl.ds(first, width)] = by_high[:rows] + (by_high[rows:] + by_low)

        launch(chunk, step)

    def fold(product, width):
        small = product[:rows, width:] + (product[rows:, :width] + product[rows:, width:])
        return product[:rows, :width] + small

    def multiply_near(chunk, step, shifts=(0, 1, 3)):
        first, width = chunks[chunk]

        for half in range(2):
            product = 0.0
            for shift in shifts:
                inner = pl.ds(pl.multiple_of(lax.rem(row + shift, RING) * depth, depth), depth)
                both = a_two[step, half, :, :, inner].reshape(2 * rows, depth)
                product += jnp.dot(both, b_two[inner, pl.ds(2 * first, 2 * width)], preferred_element_type=jnp.float32)
            total = fold(product, width)
            if shifts == (2,):
                total += part[step, half, :, pl.ds(first, width)]
            part[step, half, :, pl.ds(first, width)] = total

    def multiply_far(chunk, step):
        multiply_near(chunk, step, (2,))
        launch(chunk, step)

    def launch(chunk, step):
        if step == 0:
            for group in groups(chunk)[: 1 if chunk == len(chunks) - 1 else 2]:
                far(chunk, group)
        if step == 2:
            near(chunk, 2, groups(chunk)[0])

    def far(chunk, group):
        turn, half = group
        cols = c_cols(chunk)
        for way, device in enumerate((z_up, z_down)):
            go(remote(
                part.at[0, half, bands[way], cols], hop_two.at[half, bands[way], cols],
                two_s, two_r.at[place_of(chunk, turn), way], device,
            ))

    def near(chunk, step, group, ways=(0, 1)):
        turn, half = group
        cols = c_cols(chunk)
        for way in ways:
            band, device = bands[way if step == 1 else 1 - way], (z_up, z_down)[way]
            go(remote(
                part.at[step, half, band, cols], hop_one.at[way, half, band, cols],
                one_s, one_r.at[place_of(chunk, turn)], device,
            ))

    def add(chunk, turn=0):
        group = groups(chunk)[turn]
        half, cols = group[1], c_cols(chunk)
        for way in range(2):
            arrived(hop_two.at[half, bands[way], cols], two_r.at[place_of(chunk, turn), way])
            part[1, half, bands[way], cols] += hop_two[half, bands[way], cols]
            near(chunk, 1, group, (way,))

    def out_cols(chunk, side):
        first, width = chunks[chunk]
        return out.at[:, pl.ds(pl.multiple_of(side * columns + first, 128), width)]

    def finish(chunk, turn=0):
        cols = c_cols(chunk)
        half = groups(chunk)[turn][1]
        arrived(hop_one.at[:, half, :, cols], one_r.at[place_of(chunk, turn)])
        final[half, :, cols] = part[3, half, :, cols] + hop_one[0, half, :, cols] + hop_one[1, half, :, cols]
        if turn == 0:
            go(remote(final.at[1 - high_y, :, cols], out_cols(chunk, high_y), swap_s, swap_r, y_across))
        if turn == len(groups(chunk)) - 1:
            pltpu.make_async_copy(final.at[high_y, :, cols], out_cols(chunk, high_y), keep).start()

    def settle():
        quarter = pl.ds(0, depth)
        left(a_buf.at[:, :, :, quarter], a_y_s)
        left(a_buf.at[:, :, :, quarter], a_core_s)
        left(a_buf.at[:, :, :, quarter], a_relay_s)
        left(b_buf.at[pl.ds(0, 2 * depth)], b_s)
        left(b_buf.at[quarter], b_relay_s)
        left(part.at[0], two_s)
        left(part.at[pl.ds(0, 2)], one_s)
        left(final.at[0], swap_s)
        mine = out.at[:, pl.ds(pl.multiple_of(high_y * columns, 128), columns)]
        theirs = out.at[:, pl.ds(pl.multiple_of((1 - high_y) * columns, 128), columns)]
        pltpu.make_async_copy(final.at[high_y], mine, keep).wait()
        arrived(theirs, swap_r)

    barrier = pltpu.get_barrier_semaphore()
    peers = (x_up, x_down, y_up, y_down, z_up, z_down, y_across, twin)
    for peer in peers:
        pl.semaphore_signal(barrier, inc=1, device_id=peer, device_id_type=MESH)
    pl.semaphore_wait(barrier, len(peers))

    b_start(0, 0)
    b_start(0, 1)
    b_start(1, 0)
    a_start(0)
    a_start(1)
    a_start(2)
    a_start(3)
    b_keep()

    b_relay(0)
    b_start(1, 1)
    b_start(2, 0)
    a_relay(0, 0)
    a_relay(0, 1)
    b_relay(1)
    b_start(2, 1)
    b_start(3, 0)
    a_split(0)
    b_split(0)
    multiply(0, 0)
    a_relay(1, 0)
    a_relay(1, 1)
    b_relay(2)
    b_start(3, 1)
    b_start(4, 0)
    b_split(1)
    multiply(1, 0)
    a_split(1)
    multiply(0, 1)
    add(0)
    a_relay(2, 0)
    multiply(1, 1)
    b_relay(3)
    b_start(4, 1)
    a_relay(2, 1)
    add(1)
    a_split(2)
    multiply(0, 2)
    multiply(1, 2)
    a_relay(3, 0)
    b_split(2)
    multiply(2, 0)
    multiply(2, 1)
    multiply(2, 2)
    a_relay(3, 1)
    b_relay(4)
    b_start(5, 0)
    b_start(5, 1)
    a_split(3)
    multiply(0, 3)
    add(2)
    b_split(3)
    multiply(3, 0)
    multiply(3, 1)
    multiply(3, 2)
    multiply(1, 3)
    finish(0)
    b_split(4)
    multiply(4, 0)
    multiply(4, 1)
    add(3)
    b_relay(5)
    multiply(4, 2)
    near(4, 2, groups(4)[1])
    finish(1)
    multiply(2, 3)
    finish(2)
    multiply(3, 3)
    b_split_near(5)
    multiply_near(5, 0)
    b_split_far(5)
    multiply_far(5, 0)
    add(4, 0)
    multiply(5, 1)
    multiply(5, 2)
    finish(3)
    multiply(4, 3)
    add(5, 0)
    far(5, groups(5)[1])
    add(4, 1)
    near(5, 2, groups(5)[1])
    finish(4, 0)
    multiply(5, 3)
    finish(5, 0)
    add(5, 1)
    finish(4, 1)
    finish(5, 1)

    settle()


def per_device(left_factor, right_factor):
    layers = lax.axis_size("layer")
    rows = left_factor.shape[0] // layers
    depth = left_factor.shape[1] // RING
    full_depth = left_factor.shape[1]
    columns = right_factor.shape[1] // 2
    count = len(WIDTHS)
    dma = pltpu.SemaphoreType.DMA
    f32, bf16 = jnp.float32, jnp.bfloat16
    return pl.pallas_call(
        kernel,
        out_shape=pltpu.VMEM((rows, 2 * columns), f32),
        in_specs=[pl.BlockSpec(memory_space=pl.ANY)] * 2,
        out_specs=pl.BlockSpec(memory_space=pl.ANY),
        scratch_shapes=[
            pltpu.VMEM((4, 2, rows, full_depth), f32),
            pltpu.VMEM((4, 2, 2, rows, full_depth), bf16),
            pltpu.VMEM((full_depth, columns), f32),
            pltpu.VMEM((full_depth, 2 * columns), bf16),
            pltpu.VMEM((4, 2, rows, columns), f32),
            pltpu.VMEM((2, rows, columns), f32),
            pltpu.VMEM((2, 2, rows, columns), f32),
            pltpu.VMEM((2, rows, columns), f32),
            dma(()), dma(()), dma((4,)), dma(()), dma((4, 2, 2)), dma(()), dma((4,)),
            dma(()), dma(()), dma((count, 2)), dma((count + 1,)), dma(()),
            dma(()), dma((count + 2, 2)), dma(()), dma((count + 2,)), dma(()), dma(()), dma(()),
        ],
        compiler_params=pltpu.CompilerParams(
            collective_id=0, has_side_effects=True, vmem_limit_bytes=60000 * 1024
        ),
        name="product",
    )(left_factor, right_factor)


def solution(mesh):
    placed = (P("row", "col"), P("row", "col"))
    return jax.shard_map(
        per_device,
        mesh=mesh,
        in_specs=placed,
        out_specs=P(("row", "layer"), "col"),
        check_vma=False,
    )
```

```python
import functools

import jax
import jax.numpy as jnp
from jax import lax
from jax.experimental import pallas as pl
from jax.experimental.pallas import tpu as pltpu
from jax.sharding import PartitionSpec as P

MESH = pl.DeviceIdType.MESH
RING = 4
WIDTHS = (128,) * 6


def split(x):
    high = x.astype(jnp.bfloat16)
    low = (x - high.astype(jnp.float32)).astype(jnp.bfloat16)
    return high, low


def kernel(
    a_hbm, b_hbm, out,
    a_buf, a_two, b_buf, b_two, part, hop_two, hop_one, final,
    a_local, a_core_s, a_core_r, a_y_s, a_y_r, a_relay_s, a_relay_r,
    b_local, b_s, b_first, b_rest, b_relay_s,
    two_s, two_r, one_s, one_r, swap_s, swap_r, keep,
):
    row, col, layer = lax.axis_index("row"), lax.axis_index("col"), lax.axis_index("layer")
    low_y, core = lax.div(col, 2), lax.rem(col, 2)
    high_y, z = lax.div(layer, RING), lax.rem(layer, RING)
    y = high_y * 2 + low_y

    def on_y(at):
        return (row, lax.rem(at, 2) * 2 + core, lax.div(at, 2) * RING + z)

    x_up = (lax.rem(row + 1, RING), col, layer)
    x_down = (lax.rem(row + RING - 1, RING), col, layer)
    y_up, y_down = on_y(lax.rem(y + 1, RING)), on_y(lax.rem(y + RING - 1, RING))
    z_up = (row, col, high_y * RING + lax.rem(z + 1, RING))
    z_down = (row, col, high_y * RING + lax.rem(z + RING - 1, RING))
    y_across = (row, col, (1 - high_y) * RING + z)
    twin = (row, low_y * 2 + 1 - core, layer)

    rows = part.shape[2]
    depth = b_buf.shape[0] // RING
    half_depth = depth // 2
    columns = b_buf.shape[1]
    chunks = []
    at = 0
    for width in WIDTHS:
        chunks.append((at, width))
        at += width
    assert at == columns

    def remote(src, dst, send, recv, device):
        return pltpu.make_async_remote_copy(
            src_ref=src, dst_ref=dst, send_sem=send, recv_sem=recv, device_id=device, device_id_type=MESH
        )

    def arrived(ref, semaphore):
        remote(ref, ref, semaphore, semaphore, twin).wait_recv()

    def left(ref, semaphore):
        remote(ref, ref, semaphore, semaphore, twin).wait_send()

    def go(copy):
        copy.start()

    owners = [[lax.rem(z + shift, RING) for shift in shifts] for shifts in ((2, 2), (1, 3), (3, 1), (0, 0))]
    tall = rows // 2
    bands = (pl.ds(0, tall), pl.ds(tall, tall))
    k_at = pl.multiple_of(z * depth, depth)

    def a_source(step, half, band):
        first = half * RING * rows + owners[step][band] * rows + band * tall
        return a_hbm.at[pl.ds(pl.multiple_of(first, tall), tall), pl.ds(k_at, depth)]

    def a_place(step, half, band, quarter):
        return a_buf.at[step, half, band, pl.ds(pl.multiple_of(quarter * depth, depth), depth)]

    far_same = (1 - low_y) * 2 + core
    far_twin = (1 - low_y) * 2 + 1 - core
    near_twin = low_y * 2 + 1 - core

    def a_start(step):
        for band in range(2):
            for half, device in ((0, y_up), (1, y_down)):
                source, place = a_source(step, half, band), a_place(step, half, bands[band], col)
                go(remote(source, place, a_y_s, a_y_r.at[step, band], device))
                go(pltpu.make_async_copy(source, place, a_local))
                go(remote(source, place, a_core_s, a_core_r.at[step], twin))

    def a_relay(step, band):
        arrived(a_place(step, slice(None), bands[band], far_same), a_y_r.at[step, band])
        for half in range(2):
            here = a_place(step, half, bands[band], far_same)
            go(remote(here, here, a_relay_s, a_relay_r.at[step], twin))

    def a_split(step):
        if step == 0:
            here = a_buf.at[:, :, :, pl.ds(0, depth)]
            pltpu.make_async_copy(here, here, a_local).wait()
        arrived(a_place(step, slice(None), slice(None), near_twin), a_core_r.at[step])
        arrived(a_place(step, slice(None), slice(None), far_twin), a_relay_r.at[step])
        for half in range(2):

            @pl.loop(0, rows // 16)
            def _(tile):
                band = pl.ds(pl.multiple_of(tile * 16, 16), 16)
                high, low = split(a_buf[step, half, band, :])
                a_two[step, half, 0, band, :] = high
                a_two[step, half, 1, band, :] = low

    def b_source(chunk, part_of):
        first, width = chunks[chunk]
        return b_hbm.at[
            pl.ds(pl.multiple_of(z * depth + part_of * half_depth, half_depth), half_depth),
            pl.ds(pl.multiple_of(high_y * columns + first, 128), width),
        ]

    def b_place(chunk, part_of, quarter):
        first, width = chunks[chunk]
        return b_buf.at[
            pl.ds(pl.multiple_of(quarter * depth + part_of * half_depth, half_depth), half_depth), pl.ds(first, width)
        ]

    row_up, row_down = x_up[0], x_down[0]
    row_across = lax.rem(row + 2, RING)

    def b_own():
        source = b_hbm.at[
            pl.ds(pl.multiple_of(z * depth, depth), depth), pl.ds(pl.multiple_of(high_y * columns, 128), columns)
        ]
        place = b_buf.at[pl.ds(pl.multiple_of(row * depth, depth), depth), :]
        return pltpu.make_async_copy(source, place, b_local)

    def b_keep():
        b_own().start()

    def b_start(chunk, turn):
        for way, part_of, device in ((0, turn, x_up), (1, 1 - turn, x_down)):
            arrival = b_first.at[chunk] if turn == 0 else b_rest.at[chunk]
            go(remote(b_source(chunk, part_of), b_place(chunk, part_of, row), b_s, arrival, device))

    def b_relay(chunk):
        first, width = chunks[chunk]
        arrived(b_buf.at[pl.ds(0, depth), pl.ds(first, width)], b_first.at[chunk])
        for way, quarter, device in ((0, row_down, x_up), (1, row_up, x_down)):
            here = b_place(chunk, way, quarter)
            go(remote(here, here, b_relay_s, b_rest.at[chunk + chunk // (len(chunks) - 1)], device))

    def b_bands(chunk, shifts):
        first, width = chunks[chunk]
        for shift in shifts:
            start = lax.rem(row + shift, RING) * depth

            @pl.loop(0, depth // 64)
            def _(tile):
                band = pl.ds(pl.multiple_of(start + tile * 64, 64), 64)
                high, low = split(b_buf[band, pl.ds(first, width)])
                b_two[band, pl.ds(2 * first, width)] = high
                b_two[band, pl.ds(2 * first + width, width)] = low

    def b_split_near(chunk):
        first, width = chunks[chunk]
        arrived(b_buf.at[pl.ds(0, depth), pl.ds(first, width)], b_rest.at[chunk])
        b_bands(chunk, (0, 1, 3))

    def b_split_far(chunk):
        first, width = chunks[chunk]
        arrived(b_buf.at[pl.ds(0, depth), pl.ds(first, width)], b_rest.at[chunk + 1])
        b_bands(chunk, (2,))

    def b_split(chunk):
        first, width = chunks[chunk]
        if chunk == 0:
            b_own().wait()
        arrived(b_buf.at[pl.ds(0, 2 * depth), pl.ds(first, width)], b_rest.at[chunk])
        b_bands(chunk, range(RING))

    def place_of(chunk, turn):
        return chunk + turn + max(0, chunk - (len(chunks) - 2))

    def c_cols(chunk):
        first, width = chunks[chunk]
        return pl.ds(first, width)

    def groups(chunk):
        return ((0, 1 - high_y), (1, high_y)) if chunk >= len(chunks) - 2 else ((0, slice(None)),)

    def multiply(chunk, step):
        first, width = chunks[chunk]

        for half in range(2):
            both = a_two[step, half].reshape(2 * rows, -1)
            if width % 256:
                product = jnp.dot(both, b_two[:, pl.ds(2 * first, 2 * width)], preferred_element_type=jnp.float32)
                part[step, half, :, pl.ds(first, width)] = fold(product, width)
            else:
                by_high = jnp.dot(both, b_two[:, pl.ds(2 * first, width)], preferred_element_type=jnp.float32)
                by_low = jnp.dot(
                    a_two[step, half, 0], b_two[:, pl.ds(2 * first + width, width)], preferred_element_type=jnp.float32
                )
                part[step, half, :, pl.ds(first, width)] = by_high[:rows] + (by_high[rows:] + by_low)

        launch(chunk, step)

    def fold(product, width):
        small = product[:rows, width:] + (product[rows:, :width] + product[rows:, width:])
        return product[:rows, :width] + small

    def multiply_near(chunk, step, shifts=(0, 1, 3)):
        first, width = chunks[chunk]

        for half in range(2):
            product = 0.0
            for shift in shifts:
                inner = pl.ds(pl.multiple_of(lax.rem(row + shift, RING) * depth, depth), depth)
                both = a_two[step, half, :, :, inner].reshape(2 * rows, depth)
                product += jnp.dot(both, b_two[inner, pl.ds(2 * first, 2 * width)], preferred_element_type=jnp.float32)
            total = fold(product, width)
            if shifts == (2,):
                total += part[step, half, :, pl.ds(first, width)]
            part[step, half, :, pl.ds(first, width)] = total

    def multiply_far(chunk, step):
        multiply_near(chunk, step, (2,))
        launch(chunk, step)

    def launch(chunk, step):
        if step == 0:
            for group in groups(chunk)[: 1 if chunk == len(chunks) - 1 else 2]:
                far(chunk, group)
        if step == 2:
            near(chunk, 2, groups(chunk)[0])

    def far(chunk, group):
        turn, half = group
        cols = c_cols(chunk)
        for way, device in enumerate((z_up, z_down)):
            go(remote(
                part.at[0, half, bands[way], cols], hop_two.at[half, bands[way], cols],
                two_s, two_r.at[place_of(chunk, turn), way], device,
            ))

    def near(chunk, step, group, ways=(0, 1)):
        turn, half = group
        cols = c_cols(chunk)
        for way in ways:
            band, device = bands[way if step == 1 else 1 - way], (z_up, z_down)[way]
            go(remote(
                part.at[step, half, band, cols], hop_one.at[way, half, band, cols],
                one_s, one_r.at[place_of(chunk, turn)], device,
            ))

    def add(chunk, turn=0):
        group = groups(chunk)[turn]
        half, cols = group[1], c_cols(chunk)
        for way in range(2):
            arrived(hop_two.at[half, bands[way], cols], two_r.at[place_of(chunk, turn), way])
            part[1, half, bands[way], cols] += hop_two[half, bands[way], cols]
            near(chunk, 1, group, (way,))

    def out_cols(chunk, side):
        first, width = chunks[chunk]
        return out.at[:, pl.ds(pl.multiple_of(side * columns + first, 128), width)]

    def finish(chunk, turn=0):
        cols = c_cols(chunk)
        half = groups(chunk)[turn][1]
        arrived(hop_one.at[:, half, :, cols], one_r.at[place_of(chunk, turn)])
        final[half, :, cols] = part[3, half, :, cols] + hop_one[0, half, :, cols] + hop_one[1, half, :, cols]
        if turn == 0:
            go(remote(final.at[1 - high_y, :, cols], out_cols(chunk, high_y), swap_s, swap_r, y_across))
        if turn == len(groups(chunk)) - 1:
            pltpu.make_async_copy(final.at[high_y, :, cols], out_cols(chunk, high_y), keep).start()

    def settle():
        quarter = pl.ds(0, depth)
        left(a_buf.at[:, :, :, quarter], a_y_s)
        left(a_buf.at[:, :, :, quarter], a_core_s)
        left(a_buf.at[:, :, :, quarter], a_relay_s)
        left(b_buf.at[pl.ds(0, 2 * depth)], b_s)
        left(b_buf.at[quarter], b_relay_s)
        left(part.at[0], two_s)
        left(part.at[pl.ds(0, 2)], one_s)
        left(final.at[0], swap_s)
        mine = out.at[:, pl.ds(pl.multiple_of(high_y * columns, 128), columns)]
        theirs = out.at[:, pl.ds(pl.multiple_of((1 - high_y) * columns, 128), columns)]
        pltpu.make_async_copy(final.at[high_y], mine, keep).wait()
        arrived(theirs, swap_r)

    barrier = pltpu.get_barrier_semaphore()
    peers = (x_up, x_down, y_up, y_down, z_up, z_down, y_across, twin)
    for peer in peers:
        pl.semaphore_signal(barrier, inc=1, device_id=peer, device_id_type=MESH)
    pl.semaphore_wait(barrier, len(peers))

    b_start(0, 0)
    b_start(0, 1)
    b_start(1, 0)
    a_start(0)
    a_start(1)
    a_start(2)
    a_start(3)
    b_keep()

    b_relay(0)
    b_start(1, 1)
    b_start(2, 0)
    a_relay(0, 0)
    a_relay(0, 1)
    b_relay(1)
    b_start(2, 1)
    b_start(3, 0)
    a_split(0)
    b_split(0)
    multiply(0, 0)
    a_relay(1, 0)
    a_relay(1, 1)
    b_relay(2)
    b_start(3, 1)
    b_start(4, 0)
    b_split(1)
    multiply(1, 0)
    a_split(1)
    multiply(0, 1)
    add(0)
    a_relay(2, 0)
    multiply(1, 1)
    b_relay(3)
    b_start(4, 1)
    a_relay(2, 1)
    add(1)
    a_split(2)
    multiply(0, 2)
    multiply(1, 2)
    a_relay(3, 0)
    b_split(2)
    multiply(2, 0)
    multiply(2, 1)
    multiply(2, 2)
    a_relay(3, 1)
    b_relay(4)
    b_start(5, 0)
    b_start(5, 1)
    a_split(3)
    multiply(0, 3)
    add(2)
    b_split(3)
    multiply(3, 0)
    multiply(3, 1)
    multiply(3, 2)
    multiply(1, 3)
    finish(0)
    b_split(4)
    multiply(4, 0)
    multiply(4, 1)
    add(3)
    b_relay(5)
    multiply(4, 2)
    near(4, 2, groups(4)[1])
    finish(1)
    multiply(2, 3)
    finish(2)
    multiply(3, 3)
    b_split_near(5)
    multiply_near(5, 0)
    b_split_far(5)
    multiply_far(5, 0)
    add(4, 0)
    multiply(5, 1)
    multiply(5, 2)
    finish(3)
    multiply(4, 3)
    add(5, 0)
    far(5, groups(5)[1])
    add(4, 1)
    near(5, 2, groups(5)[1])
    finish(4, 0)
    multiply(5, 3)
    finish(5, 0)
    add(5, 1)
    finish(4, 1)
    finish(5, 1)

    settle()


def per_device(left_factor, right_factor):
    layers = lax.axis_size("layer")
    rows = left_factor.shape[0] // layers
    depth = left_factor.shape[1] // RING
    full_depth = left_factor.shape[1]
    columns = right_factor.shape[1] // 2
    count = len(WIDTHS)
    dma = pltpu.SemaphoreType.DMA
    f32, bf16 = jnp.float32, jnp.bfloat16
    return pl.pallas_call(
        kernel,
        out_shape=pltpu.VMEM((rows, 2 * columns), f32),
        in_specs=[pl.BlockSpec(memory_space=pl.ANY)] * 2,
        out_specs=pl.BlockSpec(memory_space=pl.ANY),
        scratch_shapes=[
            pltpu.VMEM((4, 2, rows, full_depth), f32),
            pltpu.VMEM((4, 2, 2, rows, full_depth), bf16),
            pltpu.VMEM((full_depth, columns), f32),
            pltpu.VMEM((full_depth, 2 * columns), bf16),
            pltpu.VMEM((4, 2, rows, columns), f32),
            pltpu.VMEM((2, rows, columns), f32),
            pltpu.VMEM((2, 2, rows, columns), f32),
            pltpu.VMEM((2, rows, columns), f32),
            dma(()), dma(()), dma((4,)), dma(()), dma((4, 2)), dma(()), dma((4,)),
            dma(()), dma(()), dma((count,)), dma((count + 1,)), dma(()),
            dma(()), dma((count + 2, 2)), dma(()), dma((count + 2,)), dma(()), dma(()), dma(()),
        ],
        compiler_params=pltpu.CompilerParams(
            collective_id=0, has_side_effects=True, vmem_limit_bytes=60000 * 1024
        ),
        name="product",
    )(left_factor, right_factor)


def solution(mesh):
    placed = (P("row", "col"), P("row", "col"))
    return jax.shard_map(
        per_device,
        mesh=mesh,
        in_specs=placed,
        out_specs=P(("row", "layer"), "col"),
        check_vma=False,
    )
```
